32 devices in a mesh: sector: 4 (over y, core), ops: 8 (over z, x).
Axes of the slice: x: 2, y: 2, z: 4, core: 2. Of those that a mesh axis runs over, the one named last changes fastest.
Arguments:
- wavefunction: bfloat16 [4, 1024, 1024], P('sector', 'ops'), may hold values from -6 to 6
- diag_scale: float32 [4, 1024, 1024], P('sector', 'ops'), may hold values from 1 to 8
- sector_dims: int32 [4], P('sector'), may hold values from 512 to 1024
- left_ops: bfloat16 [4, 16, 1024, 1024], P('sector', 'ops'), may hold values from -0.1875 to 0.1875
- right_ops: bfloat16 [4, 16, 1024, 1024], P('sector', 'ops'), may hold values from -0.1875 to 0.1875
- weight_index: int32 [4, 16], P('sector', 'ops'), may hold values from 0 to 15
- weight_table: float32 [16], replicated, may hold values from -1 to 1
Outputs:
- basis: bfloat16 [4, 1024, 1024], P('sector', 'ops')
- energy: float32 [4], P('sector')
- next_ops: float32 [1024, 1024], P('ops')
The draws below stay inside these ranges and needn't reach their ends.
All inputs are finite; a program needn't handle non-finite values.
Results may differ from the reference program's by a relative error of at most 0.025.
Values may be sent and summed in bfloat16 or wider, within the bound.
A program may use at most 128 MiB of HBM per device.

```python
import math
import jax
import jax.numpy as jnp
from jax import lax

K = 1024
KEEP = 1024
NW = 16
GROUPS = 4
PAIRS = 16


def set_ends(entries, stream_key, smallest, largest):
    spot = [jax.random.randint(jax.random.fold_in(stream_key, axis), (), 0, length) for axis, length in enumerate(entries.shape)]
    main_axis = entries.shape.index(max(entries.shape))
    neighbour = spot[:main_axis] + [(spot[main_axis] + 1) % entries.shape[main_axis]] + spot[main_axis + 1:]
    return entries.at[tuple(spot)].set(smallest).at[tuple(neighbour)].set(largest)


def block_levels(own_key, shape, shards, low, high):
    level = 1.0
    for axis_at, parts in shards:
        heights = jax.random.uniform(jax.random.fold_in(jax.random.fold_in(own_key, 6), axis_at), (parts,), jnp.float32, low / len(shards), high / len(shards))
        level = level * jnp.repeat(jnp.exp(heights), shape[axis_at] // parts).reshape((-1,) + (1,) * (len(shape) - 1 - axis_at))
    return level


def bell_draw(stream_key, shape, deviation, most, pieces=(), held_as=jnp.bfloat16):
    values = deviation * jax.random.normal(stream_key, shape, jnp.float32)
    if pieces:
        values = values * block_levels(stream_key, shape, pieces, -0.22, 0.18)
    return jnp.clip(values, -most, most).astype(held_as)


def setup_inputs(seed: int = 0) -> dict:
    arg_keys = jax.random.split(jax.random.key(seed), 8)
    return {
        "wavefunction": bell_draw(arg_keys[0], (GROUPS, K, K), 1.0, 6.0, ((0, 4), (1, 8))),
        "diag_scale": jnp.clip(jnp.exp(math.log(8.0) - 2.0794415 * jax.random.uniform(arg_keys[1], (GROUPS, K, K), jnp.float32) ** block_levels(arg_keys[1], (GROUPS, K, K), ((0, 4), (1, 8)), -0.2, 0.2)), 1.0, 8.0),
        "sector_dims": set_ends(jax.random.randint(arg_keys[2], (GROUPS,), K // 2, K + 1), jax.random.fold_in(arg_keys[2], 1), K // 2, K).astype(jnp.int32),
        "left_ops": bell_draw(arg_keys[3], (GROUPS, PAIRS, K, K), K ** -0.5, 0.1875, ((0, 4), (1, 8))),
        "right_ops": bell_draw(arg_keys[4], (GROUPS, PAIRS, K, K), K ** -0.5, 0.1875, ((0, 4), (1, 8))),
        "weight_index": set_ends(jax.random.randint(arg_keys[5], (GROUPS, PAIRS), 0, NW), jax.random.fold_in(arg_keys[5], 1), 0, NW - 1).astype(jnp.int32),
        "weight_table": jnp.clip(jax.random.uniform(arg_keys[6], (NW,), jnp.float32, -1.0, 1.0), -1.0, 1.0),
    }


def group_step(psi, scale, dim, left, right, index, table):
    order_k = psi.shape[0]
    rows = jnp.arange(order_k)
    live = rows < dim
    mask = live[:, None] & live[None, :]
    psi_m = jnp.where(mask, psi, jnp.zeros_like(psi))
    onehot = (index[:, None] == jnp.arange(table.shape[0])[None, :]).astype(jnp.float32)
    coef = jnp.sum(onehot * table[None, :], axis=1)

    def add_pair(total, item):
        left_p, right_p, weight = item
        applied = jnp.dot(left_p.astype(jnp.float32), psi_m.astype(jnp.float32), preferred_element_type=jnp.float32).astype(jnp.bfloat16)
        term = lax.dot_general(applied.astype(jnp.float32), right_p.astype(jnp.float32), (((1,), (1,)), ((), ())), preferred_element_type=jnp.float32)
        return (total + weight * term, None)
    sigma, _ = lax.scan(add_pair, jnp.zeros((order_k, order_k), jnp.float32), (left, right, coef))
    sigma = jnp.where(mask, sigma, jnp.float32(0.0))
    psi_f = psi_m.astype(jnp.float32)
    energy = jnp.sum(psi_f * sigma) / jnp.sum(psi_f * psi_f)
    update = psi_f + (sigma - energy * psi_f) / scale
    columns = update[:, :KEEP]
    gram = jnp.dot(columns.T, columns, precision=lax.Precision.HIGHEST) / order_k
    gram = gram + 0.001 * jnp.eye(KEEP, dtype=jnp.float32)
    factor = jnp.linalg.cholesky(gram)
    basis = jax.scipy.linalg.solve_triangular(factor, columns.T, lower=True).T.astype(jnp.bfloat16)

    def rotate_pair(total, item):
        left_p, weight = item
        moved = jnp.dot(left_p.astype(jnp.float32), basis.astype(jnp.float32), preferred_element_type=jnp.float32).astype(jnp.bfloat16)
        rotated = jnp.dot(basis.T.astype(jnp.float32), moved.astype(jnp.float32), preferred_element_type=jnp.float32) / order_k
        return (total + weight * rotated, None)
    summed, _ = lax.scan(rotate_pair, jnp.zeros((KEEP, KEEP), jnp.float32), (left, coef))
    return (basis, energy, summed)

def reference(wavefunction, diag_scale, sector_dims, left_ops, right_ops, weight_index, weight_table):

    def one_group(items):
        psi, scale, dim, left, right, index = items
        return group_step(psi, scale, dim, left, right, index, weight_table)
    basis, energy, summed = lax.map(one_group, (wavefunction, diag_scale, sector_dims, left_ops, right_ops, weight_index))
    return (basis, energy, jnp.sum(summed, axis=0))
```

```python
import functools

import jax
import jax.numpy as jnp
from jax import lax
from jax.experimental import pallas as pl
from jax.experimental.pallas import tpu as pltpu
from jax.sharding import PartitionSpec as P

BLOCK = 128
SUB = 8


def split3(u):
    high = u.astype(jnp.bfloat16).astype(jnp.float32)
    rest = u - high
    mid = rest.astype(jnp.bfloat16).astype(jnp.float32)
    low = (rest - mid).astype(jnp.bfloat16).astype(jnp.float32)
    return high, mid, low


def inverse_factor(block):
    size = block.shape[0]
    lane = lax.broadcasted_iota(jnp.int32, (SUB, size), 1)
    row = lax.broadcasted_iota(jnp.int32, (SUB, size), 0)
    below = block
    done = []
    for s in range(size // SUB):
        at = s * SUB
        top = below[:SUB]
        columns = [
            jnp.broadcast_to(top[:, at + j : at + j + 1], (SUB, size)) for j in range(SUB)
        ]
        here = (lane >= at) & (lane < at + SUB)
        body = jnp.where(here, (lane - at == row).astype(jnp.float32), top)
        pivots = jnp.ones((SUB, size), jnp.float32)
        for j in range(SUB):
            pivot = jnp.broadcast_to(columns[j][j : j + 1], (SUB, size))
            pivots = jnp.where(row == j, pivot, pivots)
            if j < SUB - 1:
                factor = jnp.where(row > j, columns[j] / pivot, 0.0)
                for c in range(j + 1, SUB):
                    columns[c] = columns[c] - factor * columns[c][j : j + 1]
                body = body - factor * body[j : j + 1]
        scaled = body * lax.rsqrt(pivots)
        done.append(scaled)
        if at + SUB < size:
            high, mid, low = split3(scaled)
            left = jnp.concatenate([high, high, mid, high, mid, low], axis=0)
            right = jnp.concatenate([high, mid, high, low, mid, high], axis=0)
            outer = lax.dot_general(
                left.T.astype(jnp.bfloat16),
                right.astype(jnp.bfloat16),
                (((1,), (0,)), ((), ())),
                preferred_element_type=jnp.float32,
            )
            rows_left = size - at - SUB
            lanes = lax.broadcasted_iota(jnp.int32, (rows_left, size), 1)
            kept = jnp.where((lanes >= at) & (lanes < at + SUB), 0.0, below[SUB:])
            below = kept - outer[at + SUB :]
    whole = jnp.concatenate(done, axis=0)
    r = lax.broadcasted_iota(jnp.int32, (size, size), 0)
    c = lax.broadcasted_iota(jnp.int32, (size, size), 1)
    return jnp.where(c <= r, whole, 0.0)


def inverse_kernel(scale, gram_ref, high_ref, low_ref, work):
    order = gram_ref.shape[0]
    blocks = order // BLOCK
    column = lax.broadcasted_iota(jnp.int32, (BLOCK, order), 1)
    local = lax.broadcasted_iota(jnp.int32, (BLOCK, order), 0)

    def rows(i):
        return pl.ds(pl.multiple_of(i * BLOCK, BLOCK), BLOCK)

    def load(i, carry):
        eye = (column == local + i * BLOCK).astype(jnp.float32)
        work[rows(i), :] = gram_ref[rows(i), :] * scale + 0.001 * eye
        return carry

    lax.fori_loop(0, blocks, load, 0)

    def step(k, carry):
        first = k * BLOCK
        inverse = inverse_factor(work[rows(k), rows(k)])
        in_k = (column >= first) & (column < first + BLOCK)
        pivot_rows = jnp.where(
            in_k, (column - first == local).astype(jnp.float32), work[rows(k), :]
        )
        work[rows(k), :] = jnp.dot(
            inverse,
            pivot_rows,
            precision=lax.Precision.HIGHEST,
            preferred_element_type=jnp.float32,
        )

        def update(i, inner):
            panel = work[rows(k), rows(i)].T
            kept = jnp.where(in_k, 0.0, work[rows(i), :])
            work[rows(i), :] = kept - jnp.dot(
                panel,
                work[rows(k), :],
                precision=lax.Precision.HIGHEST,
                preferred_element_type=jnp.float32,
            )
            return inner

        lax.fori_loop(k + 1, blocks, update, 0)
        return carry

    lax.fori_loop(0, blocks, step, 0)

    def store(i, carry):
        kept = jnp.where(column <= local + i * BLOCK, work[rows(i), :], 0.0)
        high = kept.astype(jnp.bfloat16)
        high_ref[rows(i), :] = high
        low_ref[rows(i), :] = (kept - high.astype(jnp.float32)).astype(jnp.bfloat16)
        return carry

    lax.fori_loop(0, blocks, store, 0)


def inverse_cholesky(product, scale):
    order = product.shape[0]
    half = jax.ShapeDtypeStruct((order, order), jnp.bfloat16)
    vmem = pl.BlockSpec(memory_space=pltpu.VMEM)
    return pl.pallas_call(
        functools.partial(inverse_kernel, scale),
        out_shape=(half, half),
        in_specs=[vmem],
        out_specs=(vmem, vmem),
        scratch_shapes=[pltpu.VMEM((order, order), jnp.float32)],
        compiler_params=pltpu.CompilerParams(vmem_limit_bytes=40 * 2**20),
        cost_estimate=pl.CostEstimate(
            flops=400 * order**3 // 10, bytes_accessed=8 * order**2, transcendentals=0
        ),
        name="inverse_cholesky",
    )(product)


def shards(wavefunction, diag_scale, sector_dims, left_ops, right_ops, weight_index, weight_table):
    psi_local = wavefunction[0]
    rows_dev = psi_local.shape[0]
    order_k = psi_local.shape[1]
    pair_count = left_ops.shape[1]
    owners = lax.axis_size("ops")
    first_row = lax.axis_index("ops") * rows_dev
    dim = sector_dims[0]
    live = jnp.arange(order_k) < dim
    both = live[:, None] & live[None, :]
    whole_psi = lax.all_gather(psi_local, "ops", axis=0, tiled=True)
    whole_psi = jnp.where(both, whole_psi, jnp.zeros_like(whole_psi))
    onehot = (weight_index[0][:, None] == jnp.arange(weight_table.shape[0])[None, :]).astype(
        jnp.float32
    )
    coef = jnp.sum(onehot * weight_table[None, :], axis=1)

    total = jnp.zeros((order_k, order_k), jnp.float32)
    operator = jnp.zeros((order_k, order_k), jnp.float32)
    for pair in range(pair_count):
        applied = jnp.dot(
            left_ops[0, pair], whole_psi, preferred_element_type=jnp.float32
        ).astype(jnp.bfloat16)
        term = lax.dot_general(
            applied,
            right_ops[0, pair],
            (((1,), (1,)), ((), ())),
            preferred_element_type=jnp.float32,
        )
        total = total + coef[pair] * term
        operator = operator + coef[pair] * left_ops[0, pair].astype(jnp.float32)
    total = jnp.where(both, total, jnp.float32(0.0))
    whole_f = whole_psi.astype(jnp.float32)
    partial_numer = jnp.sum(whole_f * total)
    denom = jnp.sum(whole_f * whole_f)
    packed = jnp.concatenate(
        [
            total.reshape(owners, rows_dev, order_k),
            jnp.full((owners, SUB, order_k), partial_numer),
        ],
        axis=1,
    ).reshape(owners * (rows_dev + SUB), order_k)
    summed = lax.psum_scatter(packed, "ops", scatter_dimension=0, tiled=True)
    sigma = summed[:rows_dev]
    energy = summed[rows_dev, 0] / denom

    row_live = first_row + jnp.arange(rows_dev) < dim
    psi_f = jnp.where(row_live[:, None] & live[None, :], psi_local, 0).astype(jnp.float32)
    update = psi_f + (sigma - energy * psi_f) / diag_scale[0]
    columns = lax.all_gather(update.astype(jnp.bfloat16), "ops", axis=0, tiled=True)

    operator, columns = lax.optimization_barrier((operator.astype(jnp.bfloat16), columns))
    operator = lax.psum(operator, "ops")

    product = lax.dot_general(
        columns, columns, (((0,), (0,)), ((), ())), preferred_element_type=jnp.float32
    )
    high, low = inverse_cholesky(product, 1.0 / order_k)
    across = (((1,), (1,)), ((), ()))
    basis = (
        lax.dot_general(columns, high, across, preferred_element_type=jnp.float32)
        + lax.dot_general(columns, low, across, preferred_element_type=jnp.float32)
    ).astype(jnp.bfloat16)
    basis_local = lax.dynamic_slice_in_dim(basis, first_row, rows_dev, axis=0)

    own = lax.dynamic_slice_in_dim(basis, first_row, rows_dev, axis=1)
    half = lax.dot_general(
        own, operator, (((0,), (0,)), ((), ())), preferred_element_type=jnp.float32
    ).astype(jnp.bfloat16)
    rotated = jnp.dot(half, basis, preferred_element_type=jnp.float32) / order_k
    next_rows = lax.psum(rotated.astype(jnp.bfloat16), "sector").astype(jnp.float32)
    return (basis_local[None], jnp.reshape(energy, (1,)), next_rows)


def solution(mesh):
    in_specs = (
        P("sector", "ops", None),
        P("sector", "ops", None),
        P("sector"),
        P("sector", "ops", None, None),
        P("sector", "ops", None, None),
        P("sector", "ops"),
        P(),
    )
    out_specs = (P("sector", "ops", None), P("sector"), P("ops", None))
    return jax.shard_map(shards, mesh=mesh, in_specs=in_specs, out_specs=out_specs, check_vma=False)
```
